256 devices in a mesh: wide: 16 (over z_hi, x), narrow: 4 (over y), depth: 4 (over z_lo, core).
Axes of the slice: x: 4, y: 4, z: 8 (z_hi: 4, z_lo: 2; z = z_hi * 2 + z_lo), core: 2. Of those that a mesh axis runs over, the one named last changes fastest.
Arguments:
- patch_store: bfloat16 [64, 1024, 4096], P('wide', 'depth'), may hold values from -6 to 6
- w_key: bfloat16 [4096, 1024], P(None, 'narrow'), may hold values from -0.09375 to 0.09375
- w_value: bfloat16 [4096, 1024], P(None, 'narrow'), may hold values from -0.09375 to 0.09375
- key_gain: float32 [128], replicated, may hold values from 0.1 to 1.9
- query_gain: float32 [128], replicated, may hold values from 0.1 to 1.9
- queries: bfloat16 [256, 4096], P('wide', 'narrow'), may hold values from -6 to 6
- owner_table: int32 [64], replicated, may hold values from 0 to 63, each once
- reader_table: int32 [16, 2], replicated, may hold values from 0 to 63
- request_image: int32 [256], P('wide'), may hold values from 0 to 1
- image_tiles: int32 [64], replicated, may hold values from 1 to 4
Outputs:
- context: bfloat16 [256, 4096], P(('wide', 'depth'), 'narrow')
The draws below stay inside these ranges and needn't reach their ends.
Inputs may be any that keep to these rules, and one draw needn't show every extreme that they name: owner_table is a permutation of the slots. `reader_table`: entries are image ids; a group's list may repeat an image.
All inputs are finite; a program needn't handle non-finite values.
Results may differ from the reference program's by a relative error of at most 0.012.
Values may be sent and summed in bfloat16 or wider, within the bound.
A program may use at most 64 MiB of HBM per device.

```python
import math
import jax
import jax.numpy as jnp
import numpy as np
from jax import lax

D = 4096
HEADS = 32
KV_HEADS = 8
HD = 128
TILES = 4
TILE_P = 256
READS = 2
PATCHES = 1024
IMAGES = 64
GROUPS = 16
BATCH = 256
N_WIDE = 16


def touch_ends(values, own_key, smallest, largest):
    place = [jax.random.randint(jax.random.fold_in(own_key, axis), (), 0, length) for axis, length in enumerate(values.shape)]
    main_axis = values.shape.index(max(values.shape))
    neighbour = place[:main_axis] + [(place[main_axis] + 1) % values.shape[main_axis]] + place[main_axis + 1:]
    return values.at[tuple(place)].set(smallest).at[tuple(neighbour)].set(largest)


def shard_levels(own_key, extent, split, smallest, high):
    def one(position, parts):
        heights = jax.random.uniform(jax.random.fold_in(jax.random.fold_in(own_key, 6), position), (parts,), jnp.float32, smallest / len(split), high / len(split))
        return jnp.repeat(jnp.exp(heights), extent[position] // parts).reshape((-1,) + (1,) * (len(extent) - position - 1))

    factor_of = one(*split[0])
    for cut in split[1:]:
        factor_of = factor_of * one(*cut)
    return factor_of


def rank_table(count, slope):
    portions = [(1 << 20) // math.isqrt(rank ** slope) + 1 for rank in range(1, count + 1)]
    spread = 1 + sum(portions) // (1 << 30)
    return np.cumsum(np.array([max(1, weight // spread) for weight in portions]))


def ranked_ids(key, extent, number_of, skew):
    table = rank_table(number_of, skew)
    lot = jax.random.randint(jax.random.fold_in(key, 1), extent, 0, int(table[number_of - 1]))
    standing = jnp.searchsorted(jnp.asarray(table, jnp.int32), lot, side="right")
    return jax.random.permutation(jax.random.fold_in(key, 2), number_of)[standing].astype(jnp.int32)


def centred(stream_key, shape, spread, reach, split=(), held_as=jnp.bfloat16):
    factor_of = shard_levels(stream_key, shape, split, -0.22, 0.18) if split else 1.0
    drawn = jax.random.normal(stream_key, shape, jnp.float32) * spread * factor_of
    return jnp.minimum(jnp.maximum(drawn, -reach), reach).astype(held_as)


def setup_inputs(seed: int = 0) -> dict:
    streams_of = jax.random.split(jax.random.key(seed), 11)
    return {
        "patch_store": centred(streams_of[0], (IMAGES, PATCHES, D), 1.0, 6.0, ((0, 16), (1, 4))),
        "w_key": centred(streams_of[1], (D, KV_HEADS * HD), D ** -0.5, 0.09375, ((1, 4),)),
        "w_value": centred(streams_of[2], (D, KV_HEADS * HD), D ** -0.5, 0.09375, ((1, 4),)),
        "key_gain": jnp.clip(1.0 + 0.18 * jax.random.normal(streams_of[3], (HD,), jnp.float32), 0.1, 1.9),
        "query_gain": jnp.clip(1.0 + 0.18 * jax.random.normal(streams_of[4], (HD,), jnp.float32), 0.1, 1.9),
        "queries": centred(streams_of[5], (BATCH, HEADS * HD), 1.0, 6.0, ((0, 16), (1, 4))),
        "owner_table": jax.random.permutation(streams_of[6], IMAGES).astype(jnp.int32),
        "reader_table": touch_ends(ranked_ids(streams_of[7], (GROUPS, READS), IMAGES, 1), jax.random.fold_in(streams_of[7], 3), 0, IMAGES - 1).astype(jnp.int32),
        "request_image": touch_ends(jax.random.randint(streams_of[8], (BATCH,), 0, READS), jax.random.fold_in(streams_of[8], 1), 0, READS - 1).astype(jnp.int32),
        "image_tiles": touch_ends(jax.random.randint(streams_of[9], (IMAGES,), 1, TILES + 1), jax.random.fold_in(streams_of[9], 1), 1, TILES).astype(jnp.int32),
    }


epsilon = 1e-05

def rms_scaled(tensor, scaling):
    return tensor / jnp.sqrt(lax.optimization_barrier(jnp.mean(tensor * tensor, axis=-1, keepdims=True)) + epsilon) * scaling

def reference(patch_store, w_key, w_value, key_gain, query_gain, queries, owner_table, reader_table, request_image, image_tiles):
    batch = queries.shape[0]
    per_group = batch // N_WIDE
    group_size = HEADS // KV_HEADS
    scale = 1.0 / math.sqrt(HD)

    def one_group(group_index):
        images = reader_table[group_index]
        slots = owner_table[images]
        patch_rows = patch_store[slots].reshape(READS * PATCHES, D)
        raw_keys = jnp.dot(patch_rows, w_key, preferred_element_type=jnp.float32).reshape(READS, PATCHES, KV_HEADS, HD)
        image_keys = rms_scaled(raw_keys, key_gain).astype(jnp.bfloat16)
        image_values = jnp.dot(patch_rows, w_value, preferred_element_type=jnp.float32).astype(jnp.bfloat16)
        image_values = image_values.reshape(READS, PATCHES, KV_HEADS, HD)
        first_row = (group_index * per_group).astype(jnp.int32)
        rows_here = lax.dynamic_slice_in_dim(queries, first_row, per_group, 0).astype(jnp.float32)
        normed = rms_scaled(rows_here.reshape(per_group, KV_HEADS, group_size, HD), query_gain).astype(jnp.bfloat16)
        entries = lax.dynamic_slice_in_dim(request_image, first_row, per_group, 0)
        scores = jnp.einsum('bkgd,rskd->bkgrs', normed.astype(jnp.float32), image_keys.astype(jnp.float32)) * scale
        chosen = (entries[:, None] == jnp.arange(READS, dtype=jnp.int32)[None, :]).astype(jnp.float32)
        usable = (jnp.arange(PATCHES, dtype=jnp.int32)[None, :] // TILE_P < image_tiles[images][:, None]).astype(jnp.float32)
        weights = jnp.exp(scores) * chosen[:, None, None, :, None] * usable[None, None, None]
        denominator = lax.optimization_barrier(jnp.sum(weights, axis=(3, 4)))
        numerator = jnp.einsum('bkgrs,rskd->bkgd', weights.astype(jnp.bfloat16).astype(jnp.float32), image_values.astype(jnp.float32))
        return (numerator / denominator[..., None]).astype(jnp.bfloat16).reshape(per_group, HEADS * HD)
    result = lax.map(one_group, jnp.arange(N_WIDE, dtype=jnp.int32))
    return result.reshape(batch, HEADS * HD)
```

```python
import functools
import math

import jax
import jax.numpy as jnp
from jax import lax
from jax.experimental import pallas as pl
from jax.experimental.pallas import tpu as pltpu
from jax.sharding import PartitionSpec as P

HD = 128
EPSILON = 1e-05
CHUNKS = 4
XS = 4
ZS = 8
CORES = 2
GROUP = 4
SHARE = 4
ROWS = 64
OUTSIDE = -30000.0
MESH = pl.DeviceIdType.MESH


def kernel(
    store,
    w_key,
    w_value,
    key_gain,
    query_gain,
    queries,
    owner_hbm,
    reader_hbm,
    request_hbm,
    tiles_hbm,
    out,
    owner_table,
    reader_table,
    request_image,
    image_tiles,
    xbuf,
    wbuf,
    qraw,
    gains,
    qf,
    qs,
    qx,
    ids,
    raw,
    kvout,
    kbuf,
    vbuf,
    kext,
    mnum,
    mden,
    xnum,
    xden,
    znum,
    zden,
    gnum,
    gden,
    res,
    w_sem,
    x_sem,
    small_sem,
    qz_send,
    qz_recv,
    qx_send,
    qx_recv,
    kv_send,
    kv_recv,
    rx_send,
    rx_recv,
    rz_send,
    rz_recv,
):
    images, rows, width = xbuf.shape
    batch = qraw.shape[0]
    chunk = width // CHUNKS
    pairs = ZS // 2
    wide, depth = lax.axis_index("wide"), lax.axis_index("depth")
    zh, x = wide // XS, lax.rem(wide, XS)
    zl, core = depth // CORES, lax.rem(depth, CORES)
    other = 1 - core
    z = zh * 2 + zl

    barrier = pltpu.get_barrier_semaphore()

    def x_mate(o):
        return {"wide": zh * XS + lax.rem(x + o, XS), "depth": depth}

    def z_place(dz, dc):
        there = lax.rem(z + dz, ZS)
        return there // 2, lax.rem(there, 2) * CORES + lax.rem(core + dc, CORES)

    def z_mate(dz, dc):
        pair, part = z_place(dz, dc)
        return {"wide": pair * XS + x, "depth": part}

    z_mates = [(dz, dc) for dz in range(ZS) for dc in range(CORES) if dz or dc]

    for o in range(1, XS):
        pl.semaphore_signal(barrier, inc=1, device_id=x_mate(o), device_id_type=MESH)
    for dz, dc in z_mates:
        pl.semaphore_signal(barrier, inc=1, device_id=z_mate(dz, dc), device_id_type=MESH)

    def head_lanes(which):
        return pl.ds(pl.multiple_of(which * HD, HD), HD)

    def weight_copies(slot, c):
        piece = pl.ds(c * chunk, chunk)
        which = core if slot == 0 else other
        return [
            pltpu.make_async_copy(
                source.at[piece, head_lanes(which)],
                wbuf.at[slot, piece, pl.ds(part * HD, HD)],
                w_sem.at[slot, c, part],
            )
            for part, source in enumerate((w_key, w_value))
        ]

    def patch_copy(c):
        piece = pl.ds(c * chunk, chunk)
        return pltpu.make_async_copy(store.at[:, :, piece], xbuf.at[:, :, piece], x_sem.at[c])

    mine = pl.ds(pl.multiple_of(core * GROUP * HD, HD), GROUP * HD)
    small = [
        pltpu.make_async_copy(queries.at[:, mine], qraw, small_sem.at[0]),
        pltpu.make_async_copy(query_gain, gains.at[0], small_sem.at[1]),
        pltpu.make_async_copy(key_gain, gains.at[1], small_sem.at[2]),
        pltpu.make_async_copy(owner_hbm, owner_table, small_sem.at[3]),
        pltpu.make_async_copy(reader_hbm, reader_table, small_sem.at[4]),
        pltpu.make_async_copy(request_hbm, request_image, small_sem.at[5]),
        pltpu.make_async_copy(tiles_hbm, image_tiles, small_sem.at[6]),
    ]
    for copy in small:
        copy.start()
    for c in range(CHUNKS):
        for copy in weight_copies(1, c):
            copy.start()
        patch_copy(c).start()
    for c in range(CHUNKS):
        for copy in weight_copies(0, c):
            copy.start()
    for copy in small:
        copy.wait()

    gain = gains[0] * gains[1] * (math.log2(math.e) / math.sqrt(HD))
    for h in range(GROUP):
        head = qraw[:, h * HD : (h + 1) * HD].astype(jnp.float32)
        mean = jnp.mean(head * head, axis=-1, keepdims=True)
        qf[h] = head * lax.rsqrt(mean + EPSILON) * gain
    for t in range(batch // SHARE):
        for h in range(GROUP):
            qs[pl.ds(t * 16 + h * SHARE, SHARE), :] = qf[h, pl.ds(t * SHARE, SHARE), :]
    qx[x, zh] = qs[...].astype(jnp.bfloat16)

    lane = lax.broadcasted_iota(jnp.int32, (1, HD), 1)
    request = lax.rem(lane, ROWS) // 16 * SHARE + lax.rem(lane, SHARE)
    first, second = reader_table[wide, 0], reader_table[wide, 1]
    image = jnp.zeros((1, HD), jnp.int32)
    for b in range(batch):
        image = jnp.where(request == b, jnp.where(request_image[b] == 0, first, second), image)
    ids[x, zh] = image.astype(jnp.float32)

    owner = jnp.full((1, HD), -1, jnp.int32)
    tiles = jnp.zeros((1, HD), jnp.int32)
    for m in range(owner_table.shape[0]):
        owner = jnp.where(lane == m, owner_table[m], owner)
        tiles = jnp.where(lane == m, image_tiles[m], tiles)
    for half, part in enumerate((depth, zl * CORES + other)):
        for j in range(images):
            usable = (owner == wide * images + j) & (tiles > part)
            line = jnp.where(usable, 0.0, OUTSIDE)
            kext[half, j] = jnp.broadcast_to(line, (rows, HD)).astype(jnp.bfloat16)

    def query_pieces(column, pair):
        return (qx.at[column, pair], ids.at[column, pair])

    def query_z(n):
        step = jnp.where(zl == 1, 1, pairs - 1)
        pair = lax.rem(zh + (step if n < 2 else 2), pairs)
        there = n if n < 2 else 1 - zl
        device = {"wide": pair * XS + x, "depth": there * CORES + core}
        return [
            pltpu.make_async_remote_copy(
                src_ref=ref,
                dst_ref=ref,
                send_sem=qz_send.at[n, i],
                recv_sem=qz_recv.at[zh, i],
                device_id=device,
                device_id_type=MESH,
            )
            for i, ref in enumerate(query_pieces(x, zh))
        ]

    def query_z_landed(dz):
        pair = lax.rem(zh + dz, pairs)
        return [
            pltpu.make_async_remote_copy(
                src_ref=ref,
                dst_ref=ref,
                send_sem=qz_send.at[0, i],
                recv_sem=qz_recv.at[pair, i],
                device_id=x_mate(1),
                device_id_type=MESH,
            )
            for i, ref in enumerate(query_pieces(x, pair))
        ]

    def query_x(o, dz, back=False):
        pair = lax.rem(zh + dz, pairs)
        column = lax.rem(x + (XS - o if back else 0), XS)
        return [
            pltpu.make_async_remote_copy(
                src_ref=ref,
                dst_ref=ref,
                send_sem=qx_send.at[o, dz, i],
                recv_sem=qx_recv.at[o, dz, i],
                device_id=x_mate(o),
                device_id_type=MESH,
            )
            for i, ref in enumerate(query_pieces(column, pair))
        ]

    def project_other(c):
        piece = pl.ds(c * chunk, chunk)
        part = jnp.dot(
            xbuf[:, :, piece].reshape(images * rows, chunk),
            wbuf[1, piece, :],
            preferred_element_type=jnp.float32,
        )
        raw[...] = part if c == 0 else raw[...] + part

    def normed_keys(head):
        mean = jnp.mean(head * head, axis=-1, keepdims=True)
        return (head * lax.rsqrt(mean + EPSILON)).astype(jnp.bfloat16)

    def kv_copies(j):
        return [
            pltpu.make_async_remote_copy(
                src_ref=kvout.at[part, j],
                dst_ref=into.at[1, j],
                send_sem=kv_send.at[part, j],
                recv_sem=kv_recv.at[part, j],
                device_id={"depth": zl * CORES + other},
                device_id_type=MESH,
            )
            for part, into in enumerate((kbuf, vbuf))
        ]

    for c in range(CHUNKS):
        for copy in weight_copies(1, c):
            copy.wait()
        patch_copy(c).wait()
        project_other(c)
        if c == 0:
            pl.semaphore_wait(barrier, XS - 1 + len(z_mates))
            for n in (2, 1, 0):
                for copy in query_z(n):
                    copy.start()
            for o in (2, 1, 3):
                for copy in query_x(o, 0):
                    copy.start()
    for j in range(images):
        total = raw[j * rows : (j + 1) * rows, :]
        kvout[0, j] = normed_keys(total[:, :HD])
        kvout[1, j] = total[:, HD:].astype(jnp.bfloat16)
        for copy in kv_copies(j):
            copy.start()

    for c in range(CHUNKS):
        for copy in weight_copies(0, c):
            copy.wait()
    for j in range(images):
        total = jnp.dot(xbuf[j], wbuf[0], preferred_element_type=jnp.float32)
        kbuf[0, j] = normed_keys(total[:, :HD])
        vbuf[0, j] = total[:, HD:].astype(jnp.bfloat16)

    for dz in (1, 3, 2):
        for copy in query_z_landed(dz):
            copy.wait_recv()
        for o in (2, 1, 3):
            for copy in query_x(o, dz):
                copy.start()

    for j in range(images):
        for copy in kv_copies(j):
            copy.wait_recv()

    row = lax.broadcasted_iota(jnp.int32, (HD, HD), 0)
    column_of = lax.broadcasted_iota(jnp.int32, (HD, HD), 1)
    diagonal = row == column_of
    lane_value = column_of.astype(jnp.float32)

    def attend(column):
        chosen = []
        for pair in range(pairs):
            spread = jnp.broadcast_to(ids[column, pair], (ROWS, HD))
            image = jnp.sum(
                jnp.where(diagonal[:ROWS], spread, 0.0), axis=1, keepdims=True
            )
            chosen.append(jnp.where(lane_value[:ROWS] == image, 1.0, 0.0).astype(jnp.bfloat16))
        asked = jnp.concatenate(
            [qx[column].reshape(pairs * ROWS, HD), jnp.concatenate(chosen, axis=0)], axis=1
        )
        weights, worth = [], []
        for half in range(CORES):
            for j in range(images):
                scores = lax.dot_general(
                    asked,
                    jnp.concatenate([kbuf[half, j], kext[half, j]], axis=1),
                    (((1,), (1,)), ((), ())),
                    preferred_element_type=jnp.float32,
                )
                weights.append(jnp.exp2(scores).astype(jnp.bfloat16))
                value = vbuf[half, j]
                worth.append(jnp.concatenate([value, jnp.ones_like(value)], axis=1))
        total = jnp.dot(
            jnp.concatenate(weights, axis=1),
            jnp.concatenate(worth, axis=0),
            preferred_element_type=jnp.float32,
        )
        mnum[column] = total[:, :HD].astype(jnp.bfloat16)
        for part in range(2):
            below = total[part * HD : (part + 1) * HD, HD:]
            mden[column, part] = jnp.sum(
                jnp.where(diagonal, below, 0.0), axis=0, keepdims=True
            )

    def result_x(o):
        column = lax.rem(x + o, XS)
        return [
            pltpu.make_async_remote_copy(
                src_ref=source.at[column],
                dst_ref=into.at[o],
                send_sem=rx_send.at[o, i],
                recv_sem=rx_recv.at[o, i],
                device_id=x_mate(o),
                device_id_type=MESH,
            )
            for i, (source, into) in enumerate(((mnum, xnum), (mden, xden)))
        ]

    attend(x)
    for o in (1, 3, 2):
        for dz in (0, 1, 3, 2):
            for copy in query_x(o, dz, back=True):
                copy.wait_recv()
        attend(lax.rem(x + XS - o, XS))
        for copy in result_x(XS - o):
            copy.start()

    number = mnum[x].astype(jnp.float32)
    below = mden[x]
    for o in (3, 1, 2):
        for copy in result_x(o):
            copy.wait_recv()
        number = number + xnum[o].astype(jnp.float32)
        below = below + xden[o]
    znum[...] = number.astype(jnp.bfloat16).reshape(znum.shape)
    zden[...] = below

    def result_z(dz, dc):
        pair, part = z_place(dz, dc)
        return [
            pltpu.make_async_remote_copy(
                src_ref=source,
                dst_ref=into.at[core, dz],
                send_sem=rz_send.at[dz, dc, i],
                recv_sem=rz_recv.at[dz, dc, i],
                device_id=z_mate(dz, dc),
                device_id_type=MESH,
            )
            for i, (source, into) in enumerate(
                ((znum.at[pair, part], gnum), (zden.at[pair // 2], gden))
            )
        ]

    for dz, dc in sorted(z_mates, key=lambda m: -min(m[0], ZS - m[0])):
        for copy in result_z(dz, dc):
            copy.start()
    gnum[core, 0] = znum[zh, depth]
    gden[core, 0] = zden[zh // 2]
    for dz, dc in sorted(z_mates, key=lambda m: min(m[0], ZS - m[0])):
        for copy in result_z(dz, dc):
            copy.wait_recv()

    place = lax.rem(zh, 2) * ROWS + depth * 16
    here = column_of[:16] == row[:16] + place
    for k in range(CORES):
        number = gnum[k, 0].astype(jnp.float32)
        below = gden[k, 0]
        for dz in range(1, ZS):
            number = number + gnum[k, dz].astype(jnp.float32)
            below = below + gden[k, dz]
        spread = jnp.where(here, jnp.broadcast_to(below, (16, HD)), 0.0)
        res[...] = number / jnp.sum(spread, axis=1, keepdims=True)
        for h in range(GROUP):
            out[:, pl.ds((k * GROUP + h) * HD, HD)] = res[pl.ds(h * SHARE, SHARE), :].astype(
                out.dtype
            )

    for n in range(3):
        for copy in query_z(n):
            copy.wait_send()
    for o in range(1, XS):
        for dz in range(pairs):
            for copy in query_x(o, dz):
                copy.wait_send()
        for copy in result_x(o):
            copy.wait_send()
    for j in range(images):
        for copy in kv_copies(j):
            copy.wait_send()
    for dz, dc in z_mates:
        for copy in result_z(dz, dc):
            copy.wait_send()


def local(
    patch_store,
    w_key,
    w_value,
    key_gain,
    query_gain,
    queries,
    owner_table,
    reader_table,
    request_image,
    image_tiles,
):
    images, rows, width = patch_store.shape
    batch, q_cols = queries.shape
    anywhere = pl.BlockSpec(memory_space=pl.ANY)
    dma = pltpu.SemaphoreType.DMA
    bf16, f32 = jnp.bfloat16, jnp.float32
    pairs = ZS // 2
    return pl.pallas_call(
        kernel,
        out_shape=pltpu.VMEM((SHARE, q_cols), bf16),
        in_specs=[anywhere] * 10,
        out_specs=pl.BlockSpec(memory_space=pltpu.VMEM),
        scratch_shapes=[
            pltpu.SMEM(owner_table.shape, jnp.int32),
            pltpu.SMEM(reader_table.shape, jnp.int32),
            pltpu.SMEM(request_image.shape, jnp.int32),
            pltpu.SMEM(image_tiles.shape, jnp.int32),
            pltpu.VMEM((images, rows, width), bf16),
            pltpu.VMEM((2, width, 2 * HD), bf16),
            pltpu.VMEM((batch, GROUP * HD), bf16),
            pltpu.VMEM((2, 1, HD), f32),
            pltpu.VMEM((GROUP, batch, HD), f32),
            pltpu.VMEM((ROWS, HD), f32),
            pltpu.VMEM((XS, pairs, ROWS, HD), bf16),
            pltpu.VMEM((XS, pairs, 1, HD), f32),
            pltpu.VMEM((images * rows, 2 * HD), f32),
            pltpu.VMEM((2, images, rows, HD), bf16),
            pltpu.VMEM((CORES, images, rows, HD), bf16),
            pltpu.VMEM((CORES, images, rows, HD), bf16),
            pltpu.VMEM((CORES, images, rows, HD), bf16),
            pltpu.VMEM((XS, pairs * ROWS, HD), bf16),
            pltpu.VMEM((XS, 2, 1, HD), f32),
            pltpu.VMEM((XS, pairs * ROWS, HD), bf16),
            pltpu.VMEM((XS, 2, 1, HD), f32),
            pltpu.VMEM((pairs, 2 * CORES, 16, HD), bf16),
            pltpu.VMEM((2, 1, HD), f32),
            pltpu.VMEM((CORES, ZS, 16, HD), bf16),
            pltpu.VMEM((CORES, ZS, 1, HD), f32),
            pltpu.VMEM((16, HD), f32),
            dma((2, CHUNKS, 2)),
            dma((CHUNKS,)),
            dma((7,)),
            dma((3, 2)),
            dma((pairs, 2)),
            dma((XS, pairs, 2)),
            dma((XS, pairs, 2)),
            dma((2, images)),
            dma((2, images)),
            dma((XS, 2)),
            dma((XS, 2)),
            dma((ZS, CORES, 2)),
            dma((ZS, CORES, 2)),
        ],
        compiler_params=pltpu.CompilerParams(
            collective_id=0, has_side_effects=True, vmem_limit_bytes=56 * 1024 * 1024
        ),
    )(
        patch_store,
        w_key,
        w_value,
        key_gain.reshape(1, HD),
        query_gain.reshape(1, HD),
        queries,
        owner_table,
        reader_table,
        request_image,
        image_tiles,
    )


def solution(mesh):
    placed = (
        P("wide", "depth", None),
        P(None, "narrow"),
        P(None, "narrow"),
        P(),
        P(),
        P("wide", "narrow"),
        P(),
        P(),
        P("wide"),
        P(),
    )
    return jax.shard_map(
        local,
        mesh=mesh,
        in_specs=placed,
        out_specs=P(("wide", "depth"), "narrow"),
        check_vma=False,
    )
```

```python
import functools
import math

import jax
import jax.numpy as jnp
from jax import lax
from jax.experimental import pallas as pl
from jax.experimental.pallas import tpu as pltpu
from jax.sharding import PartitionSpec as P

HD = 128
EPSILON = 1e-05
CHUNKS = 4
XS = 4
ZS = 8
CORES = 2
GROUP = 4
SHARE = 4
ROWS = 64
OUTSIDE = -30000.0
MESH = pl.DeviceIdType.MESH


def kernel(
    store,
    w_key,
    w_value,
    key_gain,
    query_gain,
    queries,
    owner_hbm,
    reader_hbm,
    request_hbm,
    tiles_hbm,
    out,
    owner_table,
    reader_table,
    request_image,
    image_tiles,
    xbuf,
    wbuf,
    qraw,
    gains,
    qf,
    qs,
    qx,
    ids,
    raw,
    kvout,
    kbuf,
    vbuf,
    kext,
    mnum,
    mden,
    xnum,
    xden,
    znum,
    zden,
    gnum,
    gden,
    res,
    w_sem,
    x_sem,
    small_sem,
    qz_send,
    qz_recv,
    qx_send,
    qx_recv,
    kv_send,
    kv_recv,
    rx_send,
    rx_recv,
    rz_send,
    rz_recv,
):
    images, rows, width = xbuf.shape
    batch = qraw.shape[0]
    chunk = width // CHUNKS
    pairs = ZS // 2
    wide, depth = lax.axis_index("wide"), lax.axis_index("depth")
    zh, x = wide // XS, lax.rem(wide, XS)
    zl, core = depth // CORES, lax.rem(depth, CORES)
    other = 1 - core
    z = zh * 2 + zl

    barrier = pltpu.get_barrier_semaphore()

    def x_mate(o):
        return {"wide": zh * XS + lax.rem(x + o, XS), "depth": depth}

    def z_mate(dz, dc):
        there = lax.rem(z + dz, ZS)
        part = lax.rem(there, 2) * CORES + lax.rem(core + dc, CORES)
        return {"wide": there // 2 * XS + x, "depth": part}

    z_mates = [(dz, dc) for dz in range(ZS) for dc in range(CORES) if dz or dc]

    for o in range(1, XS):
        pl.semaphore_signal(barrier, inc=1, device_id=x_mate(o), device_id_type=MESH)
    for dz, dc in z_mates:
        pl.semaphore_signal(barrier, inc=1, device_id=z_mate(dz, dc), device_id_type=MESH)

    def head_lanes(which):
        return pl.ds(pl.multiple_of(which * HD, HD), HD)

    def weight_copies(c):
        piece = pl.ds(c * chunk, chunk)
        return [
            pltpu.make_async_copy(
                source.at[piece, head_lanes(which)],
                wbuf.at[piece, pl.ds((2 * slot + part) * HD, HD)],
                w_sem.at[slot, c, part],
            )
            for slot, which in enumerate((core, other))
            for part, source in enumerate((w_key, w_value))
        ]

    def patch_copy(c):
        if c < CHUNKS:
            place = (pl.ds(0, 2), slice(None), pl.ds(c * chunk, chunk))
        else:
            place = (c - CHUNKS + 2,)
        return pltpu.make_async_copy(store.at[place], xbuf.at[place], x_sem.at[c])

    mine = pl.ds(pl.multiple_of(core * GROUP * HD, HD), GROUP * HD)
    small = [
        pltpu.make_async_copy(queries.at[:, mine], qraw, small_sem.at[0]),
        pltpu.make_async_copy(query_gain, gains.at[0], small_sem.at[1]),
        pltpu.make_async_copy(key_gain, gains.at[1], small_sem.at[2]),
        pltpu.make_async_copy(owner_hbm, owner_table, small_sem.at[3]),
        pltpu.make_async_copy(reader_hbm, reader_table, small_sem.at[4]),
        pltpu.make_async_copy(request_hbm, request_image, small_sem.at[5]),
        pltpu.make_async_copy(tiles_hbm, image_tiles, small_sem.at[6]),
    ]
    for copy in small:
        copy.start()
    for c in range(CHUNKS):
        for copy in weight_copies(c):
            copy.start()
        patch_copy(c).start()
    for j in range(2, images):
        patch_copy(CHUNKS + j - 2).start()
    for copy in small:
        copy.wait()

    gain = gains[0] * gains[1] * (math.log2(math.e) / math.sqrt(HD))
    for h in range(GROUP):
        head = qraw[:, h * HD : (h + 1) * HD].astype(jnp.float32)
        mean = jnp.mean(head * head, axis=-1, keepdims=True)
        qf[h] = head * lax.rsqrt(mean + EPSILON) * gain
    for t in range(batch // SHARE):
        for h in range(GROUP):
            qs[pl.ds(t * 16 + h * SHARE, SHARE), :] = qf[h, pl.ds(t * SHARE, SHARE), :]
    qx[zh, x] = qs[...].astype(jnp.bfloat16)

    lane = lax.broadcasted_iota(jnp.int32, (1, HD), 1)
    request = lax.rem(lane, ROWS) // 16 * SHARE + lax.rem(lane, SHARE)
    first, second = reader_table[0, wide], reader_table[1, wide]
    image = jnp.zeros((1, HD), jnp.int32)
    for b in range(batch):
        image = jnp.where(request == b, jnp.where(request_image[b] == 0, first, second), image)
    ids[zh, x] = image.astype(jnp.float32)

    owner = jnp.full((1, HD), -1, jnp.int32)
    tiles = jnp.zeros((1, HD), jnp.int32)
    for m in range(owner_table.shape[0]):
        owner = jnp.where(lane == m, owner_table[m], owner)
        tiles = jnp.where(lane == m, image_tiles[m], tiles)
    for half, part in enumerate((depth, zl * CORES + other)):
        for j in range(images):
            usable = (owner == wide * images + j) & (tiles > part)
            line = jnp.where(usable, 0.0, OUTSIDE)
            kext[half, j] = jnp.broadcast_to(line, (rows, HD)).astype(jnp.bfloat16)

    def query_pieces(pair, column):
        return (qx.at[pair, column], ids.at[pair, column])

    def query_z(n):
        step = jnp.where(zl == 1, 1, pairs - 1)
        pair = lax.rem(zh + (step if n < 2 else 2), pairs)
        there = n if n < 2 else 1 - zl
        device = {"wide": pair * XS + x, "depth": there * CORES + core}
        return [
            pltpu.make_async_remote_copy(
                src_ref=ref,
                dst_ref=ref,
                send_sem=qz_send.at[n, i],
                recv_sem=qz_recv.at[zh, i],
                device_id=device,
                device_id_type=MESH,
            )
            for i, ref in enumerate(query_pieces(zh, x))
        ]

    def query_z_landed(dz):
        pair = lax.rem(zh + dz, pairs)
        return [
            pltpu.make_async_remote_copy(
                src_ref=ref,
                dst_ref=ref,
                send_sem=qz_send.at[0, i],
                recv_sem=qz_recv.at[pair, i],
                device_id=x_mate(1),
                device_id_type=MESH,
            )
            for i, ref in enumerate(query_pieces(pair, x))
        ]

    def query_x(o, dz, back=False):
        pair = lax.rem(zh + dz, pairs)
        column = lax.rem(x + (XS - o if back else 0), XS)
        return [
            pltpu.make_async_remote_copy(
                src_ref=ref,
                dst_ref=ref,
                send_sem=qx_send.at[o, dz, i],
                recv_sem=qx_recv.at[o, dz, i],
                device_id=x_mate(o),
                device_id_type=MESH,
            )
            for i, ref in enumerate(query_pieces(pair, column))
        ]

    def forward(dz):
        if dz:
            for copy in query_z_landed(dz):
                copy.wait_recv()
        for o in (2, 1, 3):
            for copy in query_x(o, dz):
                copy.start()

    def project_pair(c):
        piece = pl.ds(c * chunk, chunk)
        part = jnp.dot(
            xbuf[:2, :, piece].reshape(2 * rows, chunk),
            wbuf[piece, :],
            preferred_element_type=jnp.float32,
        )
        raw[...] = part if c == 0 else raw[...] + part

    def normed_keys(head):
        mean = jnp.mean(head * head, axis=-1, keepdims=True)
        return (head * lax.rsqrt(mean + EPSILON)).astype(jnp.bfloat16)

    def kv_copies(j):
        return [
            pltpu.make_async_remote_copy(
                src_ref=kvout.at[part, j],
                dst_ref=into.at[1, j],
                send_sem=kv_send.at[part, j],
                recv_sem=kv_recv.at[part, j],
                device_id={"depth": zl * CORES + other},
                device_id_type=MESH,
            )
            for part, into in enumerate((kbuf, vbuf))
        ]

    def keep_kv(j, total):
        kvout[0, j] = normed_keys(total[:, 2 * HD : 3 * HD])
        kvout[1, j] = total[:, 3 * HD :].astype(jnp.bfloat16)
        for copy in kv_copies(j):
            copy.start()
        kbuf[0, j] = normed_keys(total[:, :HD])
        vbuf[0, j] = total[:, HD : 2 * HD].astype(jnp.bfloat16)

    def project_step(c):
        for copy in weight_copies(c):
            copy.wait()
        patch_copy(c).wait()
        project_pair(c)

    def project_image(j):
        patch_copy(CHUNKS + j - 2).wait()
        keep_kv(j, jnp.dot(xbuf[j], wbuf[...], preferred_element_type=jnp.float32))

    project_step(0)
    pl.semaphore_wait(barrier, XS - 1 + len(z_mates))
    for n in (2, 1, 0):
        for copy in query_z(n):
            copy.start()
    forward(0)
    for c in range(1, CHUNKS):
        project_step(c)
    for j in range(2):
        keep_kv(j, raw[j * rows : (j + 1) * rows, :])
    project_image(2)
    project_image(3)
    forward(1)
    forward(3)
    forward(2)
    for j in range(images):
        for copy in kv_copies(j):
            copy.wait_recv()

    row = lax.broadcasted_iota(jnp.int32, (HD, HD), 0)
    column_of = lax.broadcasted_iota(jnp.int32, (HD, HD), 1)
    diagonal = row == column_of
    lane_value = column_of.astype(jnp.float32)

    def attend(dz):
        pair = lax.rem(zh + dz, pairs)
        chosen = []
        for column in range(XS):
            spread = jnp.broadcast_to(ids[pair, column], (ROWS, HD))
            image = jnp.sum(
                jnp.where(diagonal[:ROWS], spread, 0.0), axis=1, keepdims=True
            )
            chosen.append(jnp.where(lane_value[:ROWS] == image, 1.0, 0.0).astype(jnp.bfloat16))
        asked = jnp.concatenate(
            [qx[pair].reshape(XS * ROWS, HD), jnp.concatenate(chosen, axis=0)], axis=1
        )
        weights, worth = [], []
        for half in range(CORES):
            for j in range(images):
                scores = lax.dot_general(
                    asked,
                    jnp.concatenate([kbuf[half, j], kext[half, j]], axis=1),
                    (((1,), (1,)), ((), ())),
                    preferred_element_type=jnp.float32,
                )
                weights.append(jnp.exp2(scores).astype(jnp.bfloat16))
                value = vbuf[half, j]
                worth.append(jnp.concatenate([value, jnp.ones_like(value)], axis=1))
        total = jnp.dot(
            jnp.concatenate(weights, axis=1),
            jnp.concatenate(worth, axis=0),
            preferred_element_type=jnp.float32,
        )
        mnum[dz] = total[:, :HD].astype(jnp.bfloat16).reshape(XS, ROWS, HD)
        for part in range(2):
            below = total[part * HD : (part + 1) * HD, HD:]
            mden[dz, part] = jnp.sum(
                jnp.where(diagonal, below, 0.0), axis=0, keepdims=True
            )
        for o in (2, 1, 3):
            for copy in result_x(o, dz):
                copy.start()

    def result_x(o, dz):
        column = lax.rem(x + o, XS)
        return [
            pltpu.make_async_remote_copy(
                src_ref=source,
                dst_ref=into.at[dz, o],
                send_sem=rx_send.at[dz, o, i],
                recv_sem=rx_recv.at[dz, o, i],
                device_id=x_mate(o),
                device_id_type=MESH,
            )
            for i, (source, into) in enumerate(
                ((mnum.at[dz, column], xnum), (mden.at[dz, column // 2], xden))
            )
        ]

    def query_x_wait(dz):
        for o in (1, 3, 2):
            for copy in query_x(o, dz, back=True):
                copy.wait_recv()

    flips = [(zf, cf) for zf in range(2) for cf in range(CORES)]

    def result_z(dz, zf, cf):
        pair = lax.rem(zh + dz, pairs)
        chip = lax.rem(zl + zf, 2)
        side = lax.rem(core + cf, CORES)
        part = chip * CORES + side
        return [
            pltpu.make_async_remote_copy(
                src_ref=source,
                dst_ref=into.at[core, dz, zf],
                send_sem=rz_send.at[dz, zf, cf, i],
                recv_sem=rz_recv.at[dz, zf, cf, i],
                device_id={"wide": pair * XS + x, "depth": part},
                device_id_type=MESH,
            )
            for i, (source, into) in enumerate(
                ((znum.at[dz, part], gnum), (zden.at[dz], gden))
            )
        ]

    def pass_on(dz):
        number = mnum[dz, x].astype(jnp.float32)
        below = mden[dz, x // 2]
        for o in (1, 3, 2):
            for copy in result_x(o, dz):
                copy.wait_recv()
            number = number + xnum[dz, o].astype(jnp.float32)
            below = below + xden[dz, o]
        znum[dz] = number.astype(jnp.bfloat16).reshape(2 * CORES, 16, HD)
        zden[dz] = below
        for zf, cf in flips:
            if dz or zf or cf:
                for copy in result_z(dz, zf, cf):
                    copy.start()

    query_x_wait(0)
    attend(0)
    query_x_wait(1)
    attend(1)
    query_x_wait(3)
    attend(3)
    query_x_wait(2)
    attend(2)
    pass_on(0)
    pass_on(1)
    pass_on(3)
    pass_on(2)
    gnum[core, 0, 0] = znum[0, depth]
    gden[core, 0, 0] = zden[0]
    for dz in (0, 1, 3, 2):
        for zf, cf in flips:
            if dz or zf or cf:
                for copy in result_z(dz, zf, cf):
                    copy.wait_recv()
    place = lax.rem(x, 2) * ROWS + depth * 16
    here = column_of[:16] == row[:16] + place
    for k in range(CORES):
        number = jnp.zeros((16, HD), jnp.float32)
        below = jnp.zeros((1, HD), jnp.float32)
        for dz in range(pairs):
            for zf in range(2):
                number = number + gnum[k, dz, zf].astype(jnp.float32)
                below = below + gden[k, dz, zf]
        spread = jnp.where(here, jnp.broadcast_to(below, (16, HD)), 0.0)
        res[...] = number / jnp.sum(spread, axis=1, keepdims=True)
        for h in range(GROUP):
            out[:, pl.ds((k * GROUP + h) * HD, HD)] = res[pl.ds(h * SHARE, SHARE), :].astype(
                out.dtype
            )
    for n in range(3):
        for copy in query_z(n):
            copy.wait_send()
    for dz in range(pairs):
        for o in range(1, XS):
            for copy in query_x(o, dz) + result_x(o, dz):
                copy.wait_send()
        for zf, cf in flips:
            if dz or zf or cf:
                for copy in result_z(dz, zf, cf):
                    copy.wait_send()
    for j in range(images):
        for copy in kv_copies(j):
            copy.wait_send()


def local(
    patch_store,
    w_key,
    w_value,
    key_gain,
    query_gain,
    queries,
    owner_table,
    reader_table,
    request_image,
    image_tiles,
):
    images, rows, width = patch_store.shape
    batch, q_cols = queries.shape
    anywhere = pl.BlockSpec(memory_space=pl.ANY)
    dma = pltpu.SemaphoreType.DMA
    bf16, f32 = jnp.bfloat16, jnp.float32
    pairs = ZS // 2
    return pl.pallas_call(
        kernel,
        out_shape=pltpu.VMEM((SHARE, q_cols), bf16),
        in_specs=[anywhere] * 10,
        out_specs=pl.BlockSpec(memory_space=pltpu.VMEM),
        scratch_shapes=[
            pltpu.SMEM(owner_table.shape, jnp.int32),
            pltpu.SMEM(reader_table.shape[::-1], jnp.int32),
            pltpu.SMEM(request_image.shape, jnp.int32),
            pltpu.SMEM(image_tiles.shape, jnp.int32),
            pltpu.VMEM((images, rows, width), bf16),
            pltpu.VMEM((width, 4 * HD), bf16),
            pltpu.VMEM((batch, GROUP * HD), bf16),
            pltpu.VMEM((2, 1, HD), f32),
            pltpu.VMEM((GROUP, batch, HD), f32),
            pltpu.VMEM((ROWS, HD), f32),
            pltpu.VMEM((pairs, XS, ROWS, HD), bf16),
            pltpu.VMEM((pairs, XS, 1, HD), f32),
            pltpu.VMEM((2 * rows, 4 * HD), f32),
            pltpu.VMEM((2, images, rows, HD), bf16),
            pltpu.VMEM((CORES, images, rows, HD), bf16),
            pltpu.VMEM((CORES, images, rows, HD), bf16),
            pltpu.VMEM((CORES, images, rows, HD), bf16),
            pltpu.VMEM((pairs, XS, ROWS, HD), bf16),
            pltpu.VMEM((pairs, 2, 1, HD), f32),
            pltpu.VMEM((pairs, XS, ROWS, HD), bf16),
            pltpu.VMEM((pairs, XS, 1, HD), f32),
            pltpu.VMEM((pairs, 2 * CORES, 16, HD), bf16),
            pltpu.VMEM((pairs, 1, HD), f32),
            pltpu.VMEM((CORES, pairs, 2, 16, HD), bf16),
            pltpu.VMEM((CORES, pairs, 2, 1, HD), f32),
            pltpu.VMEM((16, HD), f32),
            dma((2, CHUNKS, 2)),
            dma((CHUNKS + images - 2,)),
            dma((7,)),
            dma((3, 2)),
            dma((pairs, 2)),
            dma((XS, pairs, 2)),
            dma((XS, pairs, 2)),
            dma((2, images)),
            dma((2, images)),
            dma((pairs, XS, 2)),
            dma((pairs, XS, 2)),
            dma((pairs, 2, CORES, 2)),
            dma((pairs, 2, CORES, 2)),
        ],
        compiler_params=pltpu.CompilerParams(
            collective_id=0, has_side_effects=True, vmem_limit_bytes=56 * 1024 * 1024
        ),
    )(
        patch_store,
        w_key,
        w_value,
        key_gain.reshape(1, HD),
        query_gain.reshape(1, HD),
        queries,
        owner_table,
        reader_table.T,
        request_image,
        image_tiles,
    )


def solution(mesh):
    placed = (
        P("wide", "depth", None),
        P(None, "narrow"),
        P(None, "narrow"),
        P(),
        P(),
        P("wide", "narrow"),
        P(),
        P(),
        P("wide"),
        P(),
    )
    return jax.shard_map(
        local,
        mesh=mesh,
        in_specs=placed,
        out_specs=P(("wide", "depth"), "narrow"),
        check_vma=False,
    )
```

```python
import functools
import math

import jax
import jax.numpy as jnp
from jax import lax
from jax.experimental import pallas as pl
from jax.experimental.pallas import tpu as pltpu
from jax.sharding import PartitionSpec as P

HD = 128
EPSILON = 1e-05
CHUNKS = 4
XS = 4
ZS = 8
CORES = 2
GROUP = 4
SHARE = 4
ROWS = 64
OUTSIDE = -30000.0
MESH = pl.DeviceIdType.MESH


def kernel(
    store,
    w_key,
    w_value,
    key_gain,
    query_gain,
    queries,
    owner_hbm,
    reader_hbm,
    request_hbm,
    tiles_hbm,
    out,
    owner_table,
    reader_table,
    request_image,
    image_tiles,
    xbuf,
    wbuf,
    qraw,
    gains,
    qf,
    qs,
    qx,
    ids,
    raw,
    kvout,
    kbuf,
    vbuf,
    kext,
    mnum,
    mden,
    xnum,
    xden,
    znum,
    zden,
    gnum,
    gden,
    wide_raw,
    res,
    w_sem,
    x_sem,
    small_sem,
    qz_send,
    qz_recv,
    qx_send,
    qx_recv,
    kv_send,
    kv_recv,
    rx_send,
    rx_recv,
    rz_send,
    rz_recv,
    near_sem,
):
    images, rows, width = xbuf.shape
    batch = qraw.shape[0]
    chunk = width // CHUNKS
    pairs = ZS // 2
    wide, depth = lax.axis_index("wide"), lax.axis_index("depth")
    zh, x = wide // XS, lax.rem(wide, XS)
    zl, core = depth // CORES, lax.rem(depth, CORES)
    other = 1 - core
    z = zh * 2 + zl

    barrier = pltpu.get_barrier_semaphore()

    def x_mate(o):
        return {"wide": zh * XS + lax.rem(x + o, XS), "depth": depth}

    def z_mate(dz, dc):
        there = lax.rem(z + dz, ZS)
        part = lax.rem(there, 2) * CORES + lax.rem(core + dc, CORES)
        return {"wide": there // 2 * XS + x, "depth": part}

    toward = jnp.where(zl == 1, 1, ZS - 1)
    greeted = [x_mate(o) for o in range(1, XS)] + [
        z_mate(0, 1),
        z_mate(toward, 0),
        z_mate(2 * toward, 0),
        z_mate(3 * toward, 0),
        z_mate(ZS * 2 - 2 * toward, 0),
    ]

    for device in greeted:
        pl.semaphore_signal(barrier, inc=1, device_id=device, device_id_type=MESH)

    def head_lanes(which):
        return pl.ds(pl.multiple_of(which * HD, HD), HD)

    def weight_copies(c):
        piece = pl.ds(c * chunk, chunk)
        return [
            pltpu.make_async_copy(
                source.at[piece, head_lanes(which)],
                wbuf.at[piece, pl.ds((2 * slot + part) * HD, HD)],
                w_sem.at[slot, c, part],
            )
            for slot, which in enumerate((core, other))
            for part, source in enumerate((w_key, w_value))
        ]

    def patch_copy(c):
        if c < CHUNKS:
            place = (pl.ds(0, 2), slice(None), pl.ds(c * chunk, chunk))
        else:
            place = (c - CHUNKS + 2,)
        return pltpu.make_async_copy(store.at[place], xbuf.at[place], x_sem.at[c])

    mine = pl.ds(pl.multiple_of(core * GROUP * HD, HD), GROUP * HD)
    small = [
        pltpu.make_async_copy(queries.at[:, mine], qraw, small_sem.at[0]),
        pltpu.make_async_copy(query_gain, gains.at[0], small_sem.at[1]),
        pltpu.make_async_copy(key_gain, gains.at[1], small_sem.at[2]),
        pltpu.make_async_copy(owner_hbm, owner_table, small_sem.at[3]),
        pltpu.make_async_copy(reader_hbm, reader_table, small_sem.at[4]),
        pltpu.make_async_copy(request_hbm, request_image, small_sem.at[5]),
        pltpu.make_async_copy(tiles_hbm, image_tiles, small_sem.at[6]),
    ]
    def start_piece(c):
        for copy in weight_copies(c):
            copy.start()
        patch_copy(c).start()

    for copy in small:
        copy.start()
    start_piece(0)
    for copy in small[:3]:
        copy.wait()
    gain = gains[0] * gains[1] * (math.log2(math.e) / math.sqrt(HD))
    for h in range(GROUP):
        head = qraw[:, h * HD : (h + 1) * HD].astype(jnp.float32)
        mean = jnp.mean(head * head, axis=-1, keepdims=True)
        qf[h] = head * lax.rsqrt(mean + EPSILON) * gain
    for t in range(batch // SHARE):
        for h in range(GROUP):
            qs[pl.ds(t * 16 + h * SHARE, SHARE), :] = qf[h, pl.ds(t * SHARE, SHARE), :]
    qx[zh, x] = qs[...].astype(jnp.bfloat16)

    for c in range(1, CHUNKS):
        start_piece(c)
    for j in range(2, images):
        patch_copy(CHUNKS + j - 2).start()
    for copy in small[3:]:
        copy.wait()
    lane = lax.broadcasted_iota(jnp.int32, (1, HD), 1)
    request = lax.rem(lane, ROWS) // 16 * SHARE + lax.rem(lane, SHARE)
    first, second = reader_table[0, wide], reader_table[1, wide]
    image = jnp.zeros((1, HD), jnp.int32)
    for b in range(batch):
        image = jnp.where(request == b, jnp.where(request_image[b] == 0, first, second), image)
    ids[zh, x] = image.astype(jnp.float32)

    owner = jnp.full((1, HD), -1, jnp.int32)
    tiles = jnp.zeros((1, HD), jnp.int32)
    for m in range(owner_table.shape[0]):
        owner = jnp.where(lane == m, owner_table[m], owner)
        tiles = jnp.where(lane == m, image_tiles[m], tiles)
    for half, part in enumerate((depth, zl * CORES + other)):
        for j in range(images):
            usable = (owner == wide * images + j) & (tiles > part)
            line = jnp.where(usable, 0.0, OUTSIDE)
            kext[half, j] = jnp.broadcast_to(line, (rows, HD)).astype(jnp.bfloat16)

    def query_pieces(pair, column):
        return (qx.at[pair, column], ids.at[pair, column])

    def query_z(n):
        step = jnp.where(zl == 1, 1, pairs - 1)
        pair = lax.rem(zh + (step if n < 2 else 2), pairs)
        there = n if n < 2 else 1 - zl
        device = {"wide": pair * XS + x, "depth": there * CORES + core}
        return [
            pltpu.make_async_remote_copy(
                src_ref=ref,
                dst_ref=ref,
                send_sem=qz_send.at[n, i],
                recv_sem=qz_recv.at[zh, i],
                device_id=device,
                device_id_type=MESH,
            )
            for i, ref in enumerate(query_pieces(zh, x))
        ]

    def query_z_landed(dz):
        pair = lax.rem(zh + dz, pairs)
        return [
            pltpu.make_async_remote_copy(
                src_ref=ref,
                dst_ref=ref,
                send_sem=qz_send.at[0, i],
                recv_sem=qz_recv.at[pair, i],
                device_id=x_mate(1),
                device_id_type=MESH,
            )
            for i, ref in enumerate(query_pieces(pair, x))
        ]

    def query_x(o, dz, back=False):
        pair = lax.rem(zh + dz, pairs)
        column = lax.rem(x + (XS - o if back else 0), XS)
        return [
            pltpu.make_async_remote_copy(
                src_ref=ref,
                dst_ref=ref,
                send_sem=qx_send.at[o, dz, i],
                recv_sem=qx_recv.at[o, dz, i],
                device_id=x_mate(o),
                device_id_type=MESH,
            )
            for i, ref in enumerate(query_pieces(pair, column))
        ]

    def forward(dz):
        if dz:
            for copy in query_z_landed(dz):
                copy.wait_recv()
        for o in (2, 1, 3):
            for copy in query_x(o, dz):
                copy.start()

    def project_pair(c):
        piece = pl.ds(c * chunk, chunk)
        part = jnp.dot(
            xbuf[:2, :, piece].reshape(2 * rows, chunk),
            wbuf[piece, :],
            preferred_element_type=jnp.float32,
        )
        raw[...] = part if c == 0 else raw[...] + part

    def normed_keys(head):
        mean = jnp.mean(head * head, axis=-1, keepdims=True)
        return (head * lax.rsqrt(mean + EPSILON)).astype(jnp.bfloat16)

    def kv_copies(j):
        return [
            pltpu.make_async_remote_copy(
                src_ref=kvout.at[part, j],
                dst_ref=into.at[1, j],
                send_sem=kv_send.at[part, j],
                recv_sem=kv_recv.at[part, j],
                device_id={"depth": zl * CORES + other},
                device_id_type=MESH,
            )
            for part, into in enumerate((kbuf, vbuf))
        ]

    def keep_kv(j, total):
        kvout[0, j] = normed_keys(total[:, 2 * HD : 3 * HD])
        kvout[1, j] = total[:, 3 * HD :].astype(jnp.bfloat16)
        for copy in kv_copies(j):
            copy.start()
        kbuf[0, j] = normed_keys(total[:, :HD])
        vbuf[0, j] = total[:, HD : 2 * HD].astype(jnp.bfloat16)

    def project_step(c):
        for copy in weight_copies(c):
            copy.wait()
        patch_copy(c).wait()
        project_pair(c)

    def project_rows(j, start, count):
        return jnp.dot(
            xbuf[j, start : start + count, :], wbuf[...], preferred_element_type=jnp.float32
        )

    project_step(0)
    pl.semaphore_wait(barrier, len(greeted))
    for n in (2, 1, 0):
        for copy in query_z(n):
            copy.start()
    forward(0)
    for c in range(1, CHUNKS):
        project_step(c)
    for j in range(2):
        keep_kv(j, raw[j * rows : (j + 1) * rows, :])
    patch_copy(CHUNKS).wait()
    keep_kv(2, project_rows(2, 0, rows))
    forward(1)
    forward(3)
    patch_copy(CHUNKS + 1).wait()
    raw[:128, :] = project_rows(3, 0, 128)
    forward(2)
    pl.semaphore_signal(near_sem, inc=1, device_id=z_mate(0, 1), device_id_type=MESH)
    raw[128:256, :] = project_rows(3, 128, 128)
    keep_kv(3, raw[:256, :])

    row = lax.broadcasted_iota(jnp.int32, (HD, HD), 0)
    column_of = lax.broadcasted_iota(jnp.int32, (HD, HD), 1)
    diagonal = row == column_of
    lane_value = column_of.astype(jnp.float32)

    def asked_of(dz):
        pair = lax.rem(zh + dz, pairs)
        chosen = []
        for column in range(XS):
            spread = jnp.broadcast_to(ids[pair, column], (ROWS, HD))
            image = jnp.sum(
                jnp.where(diagonal[:ROWS], spread, 0.0), axis=1, keepdims=True
            )
            chosen.append(jnp.where(lane_value[:ROWS] == image, 1.0, 0.0).astype(jnp.bfloat16))
        return jnp.concatenate(
            [qx[pair].reshape(XS * ROWS, HD), jnp.concatenate(chosen, axis=0)], axis=1
        )

    def weigh(asked, halves):
        weights, worth = [], []
        for half in halves:
            for j in range(images):
                scores = lax.dot_general(
                    asked,
                    jnp.concatenate([kbuf[half, j], kext[half, j]], axis=1),
                    (((1,), (1,)), ((), ())),
                    preferred_element_type=jnp.float32,
                )
                weights.append(jnp.exp2(scores).astype(jnp.bfloat16))
                value = vbuf[half, j]
                worth.append(jnp.concatenate([value, jnp.ones_like(value)], axis=1))
        return jnp.dot(
            jnp.concatenate(weights, axis=1),
            jnp.concatenate(worth, axis=0),
            preferred_element_type=jnp.float32,
        )

    def send_x(dz, total):
        mnum[dz] = total[:, :HD].astype(jnp.bfloat16).reshape(XS, ROWS, HD)
        for part in range(2):
            below = total[part * HD : (part + 1) * HD, HD:]
            mden[dz, part] = jnp.sum(
                jnp.where(diagonal, below, 0.0), axis=0, keepdims=True
            )
        for o in (2, 1, 3):
            for copy in result_x(o, dz):
                copy.start()

    def attend(dz):
        send_x(dz, weigh(asked_of(dz), range(CORES)))

    def result_x(o, dz):
        column = lax.rem(x + o, XS)
        return [
            pltpu.make_async_remote_copy(
                src_ref=source,
                dst_ref=into.at[dz, o],
                send_sem=rx_send.at[dz, o, i],
                recv_sem=rx_recv.at[dz, o, i],
                device_id=x_mate(o),
                device_id_type=MESH,
            )
            for i, (source, into) in enumerate(
                ((mnum.at[dz, column], xnum), (mden.at[dz, column // 2], xden))
            )
        ]

    def query_x_wait(dz):
        for o in (1, 3, 2):
            for copy in query_x(o, dz, back=True):
                copy.wait_recv()

    flips = [(zf, cf) for zf in range(2) for cf in range(CORES)]

    def result_z(dz, zf, cf):
        pair = lax.rem(zh + dz, pairs)
        chip = lax.rem(zl + zf, 2)
        side = lax.rem(core + cf, CORES)
        part = chip * CORES + side
        return [
            pltpu.make_async_remote_copy(
                src_ref=source,
                dst_ref=into.at[core, dz, zf],
                send_sem=rz_send.at[dz, zf, cf, i],
                recv_sem=rz_recv.at[dz, zf, cf, i],
                device_id={"wide": pair * XS + x, "depth": part},
                device_id_type=MESH,
            )
            for i, (source, into) in enumerate(
                ((znum.at[dz, part], gnum), (zden.at[dz], gden))
            )
        ]

    def pass_on(dz):
        number = mnum[dz, x].astype(jnp.float32)
        below = mden[dz, x // 2]
        for o in (1, 3, 2):
            for copy in result_x(o, dz):
                copy.wait_recv()
            number = number + xnum[dz, o].astype(jnp.float32)
            below = below + xden[dz, o]
        znum[dz] = number.astype(jnp.bfloat16).reshape(2 * CORES, 16, HD)
        zden[dz] = below
        for zf, cf in flips:
            if dz or zf or cf:
                for copy in result_z(dz, zf, cf):
                    copy.start()

    query_x_wait(0)
    wide_raw[...] = weigh(asked_of(0), (0,))
    for j in range(images):
        for copy in kv_copies(j):
            copy.wait_recv()
    send_x(0, wide_raw[...] + weigh(asked_of(0), (1,)))
    query_x_wait(2)
    attend(2)
    query_x_wait(1)
    query_x_wait(3)
    attend(1)
    pl.semaphore_wait(near_sem, 1)
    pass_on(0)
    attend(3)
    pass_on(2)
    pass_on(1)
    pass_on(3)
    gnum[core, 0, 0] = znum[0, depth]
    gden[core, 0, 0] = zden[0]
    for dz in (0, 1, 3, 2):
        for zf, cf in flips:
            if dz or zf or cf:
                for copy in result_z(dz, zf, cf):
                    copy.wait_recv()
    place = lax.rem(x, 2) * ROWS + depth * 16
    here = column_of[:16] == row[:16] + place
    for k in range(CORES):
        number = jnp.zeros((16, HD), jnp.float32)
        below = jnp.zeros((1, HD), jnp.float32)
        for dz in range(pairs):
            for zf in range(2):
                number = number + gnum[k, dz, zf].astype(jnp.float32)
                below = below + gden[k, dz, zf]
        spread = jnp.where(here, jnp.broadcast_to(below, (16, HD)), 0.0)
        res[...] = number / jnp.sum(spread, axis=1, keepdims=True)
        for h in range(GROUP):
            out[:, pl.ds((k * GROUP + h) * HD, HD)] = res[pl.ds(h * SHARE, SHARE), :].astype(
                out.dtype
            )
    for n in range(3):
        for copy in query_z(n):
            copy.wait_send()
    for dz in range(pairs):
        for o in range(1, XS):
            for copy in query_x(o, dz) + result_x(o, dz):
                copy.wait_send()
        for zf, cf in flips:
            if dz or zf or cf:
                for copy in result_z(dz, zf, cf):
                    copy.wait_send()
    for j in range(images):
        for copy in kv_copies(j):
            copy.wait_send()


def local(
    patch_store,
    w_key,
    w_value,
    key_gain,
    query_gain,
    queries,
    owner_table,
    reader_table,
    request_image,
    image_tiles,
):
    images, rows, width = patch_store.shape
    batch, q_cols = queries.shape
    anywhere = pl.BlockSpec(memory_space=pl.ANY)
    dma = pltpu.SemaphoreType.DMA
    bf16, f32 = jnp.bfloat16, jnp.float32
    pairs = ZS // 2
    return pl.pallas_call(
        kernel,
        out_shape=pltpu.VMEM((SHARE, q_cols), bf16),
        in_specs=[anywhere] * 10,
        out_specs=pl.BlockSpec(memory_space=pltpu.VMEM),
        scratch_shapes=[
            pltpu.SMEM(owner_table.shape, jnp.int32),
            pltpu.SMEM(reader_table.shape[::-1], jnp.int32),
            pltpu.SMEM(request_image.shape, jnp.int32),
            pltpu.SMEM(image_tiles.shape, jnp.int32),
            pltpu.VMEM((images, rows, width), bf16),
            pltpu.VMEM((width, 4 * HD), bf16),
            pltpu.VMEM((batch, GROUP * HD), bf16),
            pltpu.VMEM((2, 1, HD), f32),
            pltpu.VMEM((GROUP, batch, HD), f32),
            pltpu.VMEM((ROWS, HD), f32),
            pltpu.VMEM((pairs, XS, ROWS, HD), bf16),
            pltpu.VMEM((pairs, XS, 1, HD), f32),
            pltpu.VMEM((2 * rows, 4 * HD), f32),
            pltpu.VMEM((2, images, rows, HD), bf16),
            pltpu.VMEM((CORES, images, rows, HD), bf16),
            pltpu.VMEM((CORES, images, rows, HD), bf16),
            pltpu.VMEM((CORES, images, rows, HD), bf16),
            pltpu.VMEM((pairs, XS, ROWS, HD), bf16),
            pltpu.VMEM((pairs, 2, 1, HD), f32),
            pltpu.VMEM((pairs, XS, ROWS, HD), bf16),
            pltpu.VMEM((pairs, XS, 1, HD), f32),
            pltpu.VMEM((pairs, 2 * CORES, 16, HD), bf16),
            pltpu.VMEM((pairs, 1, HD), f32),
            pltpu.VMEM((CORES, pairs, 2, 16, HD), bf16),
            pltpu.VMEM((CORES, pairs, 2, 1, HD), f32),
            pltpu.VMEM((XS * ROWS, 2 * HD), f32),
            pltpu.VMEM((16, HD), f32),
            dma((2, CHUNKS, 2)),
            dma((CHUNKS + images - 2,)),
            dma((7,)),
            dma((3, 2)),
            dma((pairs, 2)),
            dma((XS, pairs, 2)),
            dma((XS, pairs, 2)),
            dma((2, images)),
            dma((2, images)),
            dma((pairs, XS, 2)),
            dma((pairs, XS, 2)),
            dma((pairs, 2, CORES, 2)),
            dma((pairs, 2, CORES, 2)),
            pltpu.SemaphoreType.REGULAR,
        ],
        compiler_params=pltpu.CompilerParams(
            collective_id=0, has_side_effects=True, vmem_limit_bytes=56 * 1024 * 1024
        ),
    )(
        patch_store,
        w_key,
        w_value,
        key_gain.reshape(1, HD),
        query_gain.reshape(1, HD),
        queries,
        owner_table,
        reader_table.T,
        request_image,
        image_tiles,
    )


def solution(mesh):
    placed = (
        P("wide", "depth", None),
        P(None, "narrow"),
        P(None, "narrow"),
        P(),
        P(),
        P("wide", "narrow"),
        P(),
        P(),
        P("wide"),
        P(),
    )
    return jax.shard_map(
        local,
        mesh=mesh,
        in_specs=placed,
        out_specs=P(("wide", "depth"), "narrow"),
        check_vma=False,
    )
```
